32 devices in a mesh: sp: 16 (over z, y, x), tp: 2 (over core).
Axes of the slice: x: 2, y: 2, z: 4, core: 2. Of those that a mesh axis runs over, the one named last changes fastest.
Arguments:
- fade_rate: float32 [1, 16384, 4096], P(None, 'sp', 'tp'), may hold values from 0.2 to 2
- update_in: bfloat16 [1, 16384, 4096], P(None, 'sp', 'tp'), may hold values from -6 to 6
- norm_gain: float32 [4096], P('tp'), may hold values from 0.25 to 1.75
Outputs:
- mixed_out: bfloat16 [1, 16384, 4096], P(None, 'sp', 'tp')
The draws below stay inside these ranges and needn't reach their ends.
All inputs are finite; a program needn't handle non-finite values.
Results may differ from the reference program's by a relative error of at most 0.0011.
Values sent between devices are 32-bit elements; how exact they have to be, the bound alone decides.
A program may use at most 128 MiB of HBM per device.

```python
import jax
import jax.numpy as jnp
from jax import lax

BATCH = 1
CHANNELS = 4096
LENGTH = 16384


def steps_of(own_key, dims, split, smallest, top_value):
    def one(dim, parts):
        steps = jax.random.uniform(jax.random.fold_in(jax.random.fold_in(own_key, 6), dim), (parts,), jnp.float32, smallest / len(split), top_value / len(split))
        return jnp.repeat(jnp.exp(steps), dims[dim] // parts).reshape((-1,) + (1,) * (len(dims) - dim - 1))

    gain = one(*split[0])
    for cut in split[1:]:
        gain = gain * one(*cut)
    return gain


def normal_values(stream_key, shape, deviation, limit, pieces=(), kind=jnp.bfloat16):
    array = deviation * jax.random.normal(stream_key, shape, jnp.float32)
    if pieces:
        array = array * steps_of(stream_key, shape, pieces, -0.22, 0.18)
    return jnp.clip(array, -limit, limit).astype(kind)


def setup_inputs(seed: int = 0) -> dict:
    seeds = jax.random.split(jax.random.key(seed), 4)
    return {
        "fade_rate": jnp.clip(0.2 + 1.8 * jax.random.uniform(seeds[0], (BATCH, LENGTH, CHANNELS), jnp.float32) ** steps_of(seeds[0], (BATCH, LENGTH, CHANNELS), ((1, 16), (2, 2)), -0.2, 0.2), 0.2, 2.0),
        "update_in": normal_values(seeds[1], (BATCH, LENGTH, CHANNELS), 1.0, 6.0, ((1, 16), (2, 2))),
        "norm_gain": jnp.clip(1.0 + 0.15 * jax.random.normal(seeds[2], (CHANNELS,), jnp.float32), 0.25, 1.75),
    }


def join_pair(earlier, later):
    return (earlier[0] * later[0], later[0] * earlier[1] + later[1])

def reference(fade_rate, update_in, norm_gain):
    keep = jnp.exp(-fade_rate / LENGTH)
    push = update_in.astype(jnp.float32) * LENGTH ** (-0.5)
    forward = lax.associative_scan(join_pair, (keep, push), axis=1)[1]
    power = lax.optimization_barrier(jnp.mean(forward * forward, axis=-1, keepdims=True))
    mixed_out = (forward * lax.rsqrt(power + 1e-06) * norm_gain).astype(jnp.bfloat16)
    return mixed_out
```

```python
import functools

import jax
import jax.numpy as jnp
from jax import lax
from jax.experimental import pallas as pl
from jax.experimental.pallas import tpu as pltpu
from jax.sharding import PartitionSpec as P

MESH = pl.DeviceIdType.MESH
EPS = 1e-06


def piece_of(size, most):
    while size % most:
        most //= 2
    return most


def scan_kernel(
    n, m, length, channels, wide, rows,
    fade_hbm, update_hbm, state_ref, gain_ref,
    fade_buf, update_buf, fall_buf, tri, summary, got, squares, got_squares,
    fade_sem, update_sem, send_sem, recv_sem, sq_send_sem, sq_recv_sem,
):
    me, part = lax.axis_index("sp"), lax.axis_index("tp")
    blocks, span, _ = state_ref.shape
    pieces = span // rows

    def fetch(b):
        columns = pl.ds(pl.multiple_of(b * wide, wide), wide)
        return (
            pltpu.make_async_copy(fade_hbm.at[0, :, columns], fade_buf.at[b], fade_sem.at[b]),
            pltpu.make_async_copy(update_hbm.at[0, :, columns], update_buf.at[b], update_sem.at[b]),
        )

    ahead = min(3, blocks)
    for b in range(ahead):
        for copy in fetch(b):
            copy.start()

    barrier = pltpu.get_barrier_semaphore()

    @pl.loop(1, n)
    def _(step):
        other = lax.rem(me + step, n)
        pl.semaphore_signal(barrier, inc=1, device_id=(other, part), device_id_type=MESH)

    for step in range(1, m):
        other = lax.rem(part + step, m)
        pl.semaphore_signal(barrier, inc=1, device_id=(me, other), device_id_type=MESH)

    later = lax.broadcasted_iota(jnp.int32, (rows, rows), 0)
    sooner = lax.broadcasted_iota(jnp.int32, (rows, rows), 1)
    tri[...] = jnp.where(sooner <= later, 1.0, 0.0).astype(jnp.bfloat16)
    pl.semaphore_wait(barrier, n - 1 + m - 1)

    def tell(b, other):
        return pltpu.make_async_remote_copy(
            src_ref=summary.at[b],
            dst_ref=got.at[me, b],
            send_sem=send_sem.at[b, other],
            recv_sem=recv_sem.at[b, me],
            device_id=(other, part),
            device_id_type=MESH,
        )

    def dot(a, b):
        return jnp.dot(a, b, preferred_element_type=jnp.float32)

    @pl.loop(0, blocks)
    def _(b):
        for copy in fetch(b):
            copy.wait()

        @pl.when(b + ahead < blocks)
        def _():
            for copy in fetch(b + ahead):
                copy.start()

        total_fall = jnp.ones((1, wide), jnp.float32)
        total = jnp.zeros((1, wide), jnp.float32)
        for k in range(pieces):
            here = pl.ds(k * rows, rows)
            fade = fade_buf[b, here, :]
            coarse = fade.astype(jnp.bfloat16)
            fine = (fade - coarse.astype(jnp.float32)).astype(jnp.bfloat16)
            faded = dot(tri[...], coarse) + dot(tri[...], fine)
            push = update_buf[b, here, :]
            growth = jnp.exp(faded * (1.0 / length))
            extra = (push.astype(jnp.float32) * (growth - 1.0)).astype(jnp.bfloat16)
            grown = dot(tri[...], push) + dot(tri[...], extra)
            fall = jnp.exp(faded * (-1.0 / length))
            fall_buf[b, here, :] = fall
            state_ref[b, here, :] = grown
            last_fall = fall[rows - 1 : rows, :]
            total = last_fall * (grown[rows - 1 : rows, :] + total)
            total_fall = total_fall * last_fall
        summary[b, 0:1, :] = total_fall
        summary[b, 1:2, :] = total

        @pl.loop(me + 1, n)
        def _(other):
            tell(b, other).start()

    def take(other, state):
        fresh = []
        for b in range(blocks):
            pltpu.make_async_remote_copy(
                src_ref=summary.at[b],
                dst_ref=got.at[other, b],
                send_sem=send_sem.at[b, other],
                recv_sem=recv_sem.at[b, other],
                device_id=(other, part),
                device_id_type=MESH,
            ).wait_recv()
            fresh.append(got[other, b, 0:1, :] * state[b] + got[other, b, 1:2, :])
        return tuple(fresh)

    entering = lax.fori_loop(
        0, me, take, tuple(jnp.zeros((1, wide), jnp.float32) for _ in range(blocks))
    )

    def share(k, step):
        other = lax.rem(part + step, m)
        return pltpu.make_async_remote_copy(
            src_ref=squares.at[k],
            dst_ref=got_squares.at[step - 1, k],
            send_sem=sq_send_sem.at[step - 1, k],
            recv_sem=sq_recv_sem.at[step - 1, k],
            device_id=(me, other),
            device_id_type=MESH,
        )

    def finish(k, entering):
        here = pl.ds(pl.multiple_of(k * rows, rows), rows)
        square = jnp.zeros((rows, 128), jnp.float32)
        leaving = []
        for b in range(blocks):
            state = fall_buf[b, here, :] * (state_ref[b, here, :] + entering[b])
            state_ref[b, here, :] = state
            for c in range(wide // 128):
                part_state = state[:, c * 128 : (c + 1) * 128]
                square = square + part_state * part_state
            leaving.append(state[rows - 1 : rows, :])
        squares[k] = square
        for step in range(1, m):
            share(k, step).start()
        return tuple(leaving)

    lax.fori_loop(0, pieces, finish, entering)

    @pl.loop(0, pieces)
    def _(k):
        square = squares[k]
        for step in range(1, m):
            share(k, step).wait_recv()
            square = square + got_squares[step - 1, k]
        power = jnp.sum(square, axis=1, keepdims=True) / (length * channels)
        gain = lax.rsqrt(power + EPS) * length ** (-0.5)
        here = pl.ds(pl.multiple_of(k * rows, rows), rows)
        gain_ref[here, :] = jnp.broadcast_to(gain, (rows, 128))

    @pl.loop(0, pieces)
    def _(k):
        for step in range(1, m):
            share(k, step).wait_send()

    @pl.loop(me + 1, n)
    def _(other):
        for b in range(blocks):
            tell(b, other).wait_send()


def norm_kernel(rows, state_ref, gain_ref, norm_gain_ref, out_hbm, out_buf, sem):
    blocks, span, wide = state_ref.shape
    pieces = span // rows

    def put(k):
        here = pl.ds(pl.multiple_of(k * rows, rows), rows)
        return pltpu.make_async_copy(out_buf.at[k], out_hbm.at[0, here, :], sem.at[k])

    @pl.loop(0, pieces)
    def _(k):
        here = pl.ds(pl.multiple_of(k * rows, rows), rows)
        gain = gain_ref[here, :]
        for b in range(blocks):
            for c in range(wide // 128):
                columns = pl.ds(b * wide + c * 128, 128)
                state = state_ref[b, here, pl.ds(c * 128, 128)]
                out_buf[k, :, columns] = (state * gain * norm_gain_ref[:, columns]).astype(
                    out_buf.dtype
                )
        put(k).start()

    @pl.loop(0, pieces)
    def _(k):
        put(k).wait()


def per_device(n, m, fade_rate, update_in, norm_gain):
    _, span, own = fade_rate.shape
    length, channels = span * n, own * m
    wide, rows = piece_of(own, 256), piece_of(span, 128)
    blocks, pieces = own // wide, span // rows
    f32, bf16 = jnp.float32, jnp.bfloat16
    anywhere = pl.BlockSpec(memory_space=pl.ANY)
    in_vmem = pl.BlockSpec(memory_space=pltpu.VMEM)
    dma = pltpu.SemaphoreType.DMA
    state, gain = pl.pallas_call(
        functools.partial(scan_kernel, n, m, length, channels, wide, rows),
        out_shape=(
            pltpu.VMEM((blocks, span, wide), f32),
            pltpu.VMEM((span, 128), f32),
        ),
        in_specs=[anywhere, anywhere],
        out_specs=(in_vmem, in_vmem),
        scratch_shapes=[
            pltpu.VMEM((blocks, span, wide), f32),
            pltpu.VMEM((blocks, span, wide), bf16),
            pltpu.VMEM((blocks, span, wide), f32),
            pltpu.VMEM((rows, rows), bf16),
            pltpu.VMEM((blocks, 2, wide), f32),
            pltpu.VMEM((n, blocks, 2, wide), f32),
            pltpu.VMEM((pieces, rows, 128), f32),
            pltpu.VMEM((m - 1, pieces, rows, 128), f32),
            dma((blocks,)),
            dma((blocks,)),
            dma((blocks, n)),
            dma((blocks, n)),
            dma((m - 1, pieces)),
            dma((m - 1, pieces)),
        ],
        compiler_params=pltpu.CompilerParams(
            collective_id=0, has_side_effects=True, vmem_limit_bytes=44 * 2**20
        ),
        name="scan",
    )(fade_rate, update_in)
    return pl.pallas_call(
        functools.partial(norm_kernel, rows),
        out_shape=jax.ShapeDtypeStruct((1, span, own), bf16),
        in_specs=[in_vmem, in_vmem, in_vmem],
        out_specs=anywhere,
        scratch_shapes=[pltpu.VMEM((pieces, rows, own), bf16), dma((pieces,))],
        compiler_params=pltpu.CompilerParams(vmem_limit_bytes=24 * 2**20),
        name="norm",
    )(state, gain, norm_gain.reshape(1, own))


def solution(mesh):
    placed = (P(None, "sp", "tp"), P(None, "sp", "tp"), P("tp"))
    return jax.shard_map(
        functools.partial(per_device, mesh.shape["sp"], mesh.shape["tp"]),
        mesh=mesh, in_specs=placed, out_specs=P(None, "sp", "tp"), check_vma=False,
    )
```

```python
import functools

import jax
import jax.numpy as jnp
from jax import lax
from jax.experimental import pallas as pl
from jax.experimental.pallas import tpu as pltpu
from jax.sharding import PartitionSpec as P

MESH = pl.DeviceIdType.MESH
EPS = 1e-06
AHEAD = 4
BROAD = 1024
SLICE = 256


def piece_of(size, most):
    most = min(size, most)
    while size % most:
        most //= 2
    return most


def group_of(n):
    group = 1
    while group * group < n:
        group *= 2
    return group


def scan_kernel(
    n, m, length, wide, rows, group,
    fade_hbm, update_hbm, state_ref, square_ref,
    fade_buf, update_buf, fall_buf, tri, ends, summary, near, passed, far, squares, got_squares,
    fade_sem, update_sem, near_send, near_recv, far_send, far_recv, sq_send_sem, sq_recv_sem,
):
    me, part = lax.axis_index("sp"), lax.axis_index("tp")
    blocks, span, _ = state_ref.shape
    pieces = span // rows
    lots, _, broad = fade_buf.shape
    strips, times = broad // wide, fade_sem.shape[0] // lots
    tall = span // times
    bunches = n // group
    bunch, rank = me // group, lax.rem(me, group)

    def fetch(i):
        lot, time = i // times, lax.rem(i, times)
        here = pl.ds(pl.multiple_of(time * tall, tall), tall)
        columns = pl.ds(pl.multiple_of(lot * broad, broad), broad)
        return (
            pltpu.make_async_copy(
                fade_hbm.at[0, here, columns], fade_buf.at[lot, here, :], fade_sem.at[i]
            ),
            pltpu.make_async_copy(
                update_hbm.at[0, here, columns], update_buf.at[lot, here, :], update_sem.at[i]
            ),
        )

    ahead = min(AHEAD, lots * times)
    for i in range(ahead):
        for copy in fetch(jnp.int32(i)):
            copy.start()

    barrier = pltpu.get_barrier_semaphore()
    for step in range(1, group):
        other = bunch * group + lax.rem(rank + step, group)
        pl.semaphore_signal(barrier, inc=1, device_id=(other, part), device_id_type=MESH)
    for step in range(1, bunches):
        other = lax.rem(me + step * group, n)
        pl.semaphore_signal(barrier, inc=1, device_id=(other, part), device_id_type=MESH)
    for step in range(1, m):
        other = lax.rem(part + step, m)
        pl.semaphore_signal(barrier, inc=1, device_id=(me, other), device_id_type=MESH)

    later = lax.broadcasted_iota(jnp.int32, (rows, 2 * rows), 0)
    sooner = lax.rem(lax.broadcasted_iota(jnp.int32, (rows, 2 * rows), 1), rows)
    tri[...] = jnp.where(sooner <= later, 1.0, 0.0).astype(jnp.bfloat16)

    def tell_near(b, step):
        other = bunch * group + lax.rem(rank + step, group)
        return pltpu.make_async_remote_copy(
            src_ref=summary.at[b],
            dst_ref=near.at[b, step - 1],
            send_sem=near_send.at[b, step - 1],
            recv_sem=near_recv.at[b, step - 1],
            device_id=(other, part),
            device_id_type=MESH,
        )

    def tell_far(b, other):
        return pltpu.make_async_remote_copy(
            src_ref=passed.at[b],
            dst_ref=far.at[b, bunch],
            send_sem=far_send.at[b, other],
            recv_sem=far_recv.at[b, bunch],
            device_id=(other * group + rank, part),
            device_id_type=MESH,
        )

    def hear_far(b, other):
        return pltpu.make_async_remote_copy(
            src_ref=passed.at[b],
            dst_ref=far.at[b, other],
            send_sem=far_send.at[b, other],
            recv_sem=far_recv.at[b, other],
            device_id=(lax.rem(me + group, n), part),
            device_id_type=MESH,
        )

    def dot(a, b):
        return jnp.dot(a, b, preferred_element_type=jnp.float32)

    rate = 1.4426950408889634 / length

    summary[:, 0:1, :] = jnp.ones((lots, 1, broad), jnp.float32)
    summary[:, 1:2, :] = jnp.zeros((lots, 1, broad), jnp.float32)

    @pl.loop(0, lots * times)
    def _(i):
        for copy in fetch(i):
            copy.wait()

        @pl.when(i + ahead < lots * times)
        def _():
            for copy in fetch(i + ahead):
                copy.start()

        lot, time = i // times, lax.rem(i, times)
        for strip in range(strips):
            mine = slice(strip * wide, (strip + 1) * wide)
            b = lot * strips + strip
            total_fall, total = summary[lot, 0:1, mine], summary[lot, 1:2, mine]
            for k in range(tall // rows):
                here = pl.ds(pl.multiple_of(time * tall + k * rows, rows), rows)
                fade = fade_buf[lot, here, mine]
                faded = dot(tri[:, :rows], fade.astype(jnp.bfloat16)) * rate
                last_fall = jnp.exp2(jnp.sum(fade, axis=0, keepdims=True) * -rate)
                push = update_buf[lot, here, mine]
                extra = push.astype(jnp.float32) * (jnp.exp2(faded) - 1.0)
                both = jnp.concatenate([push, extra.astype(jnp.bfloat16)], axis=0)
                grown = dot(tri[...], both)
                fall_buf[b, here, :] = jnp.exp2(-faded)
                state_ref[b, here, :] = grown
                ends[b, time * (tall // rows) + k, :, :] = last_fall
                total = last_fall * (grown[rows - 1 : rows, :] + total)
                total_fall = total_fall * last_fall
            summary[lot, 0:1, mine] = total_fall
            summary[lot, 1:2, mine] = total

        @pl.when(i == times - 1)
        def _():
            pl.semaphore_wait(barrier, group + bunches + m - 3)

        @pl.when(time == times - 1)
        def _():
            for step in range(1, group):
                tell_near(lot, step).start()

    @pl.loop(0, lots)
    def _(b):
        for step in range(1, group):
            tell_near(b, step).wait_recv()

        fall = jnp.ones((1, broad), jnp.float32)
        value = jnp.zeros((1, broad), jnp.float32)
        for place in range(group):
            one_fall, one = summary[b, 0:1, :], summary[b, 1:2, :]
            for step in range(1, group):
                came = lax.rem(rank - place + group, group) == step
                one_fall = jnp.where(came, near[b, step - 1, 0:1, :], one_fall)
                one = jnp.where(came, near[b, step - 1, 1:2, :], one)
            fall = fall * one_fall
            value = one_fall * value + one
        passed[b, 0:1, :] = fall
        passed[b, 1:2, :] = value

        @pl.loop(bunch + 1, bunches)
        def _(other):
            tell_far(b, other).start()

    def share(k, step):
        other = lax.rem(part + step, m)
        return pltpu.make_async_remote_copy(
            src_ref=squares.at[k],
            dst_ref=got_squares.at[step - 1, k],
            send_sem=sq_send_sem.at[step - 1, k],
            recv_sem=sq_recv_sem.at[step - 1, k],
            device_id=(me, other),
            device_id_type=MESH,
        )

    squares[...] = jnp.zeros_like(squares)

    @pl.loop(0, lots)
    def _(lot):
        def take(other, entering):
            hear_far(lot, other).wait_recv()
            return far[lot, other, 0:1, :] * entering + far[lot, other, 1:2, :]

        entering = lax.fori_loop(0, bunch, take, jnp.zeros((1, broad), jnp.float32))
        for place in range(group - 1):
            one_fall, one = near[lot, 0, 0:1, :], near[lot, 0, 1:2, :]
            for step in range(2, group):
                came = rank - place == step
                one_fall = jnp.where(came, near[lot, step - 1, 0:1, :], one_fall)
                one = jnp.where(came, near[lot, step - 1, 1:2, :], one)
            before = place < rank
            entering = jnp.where(before, one_fall * entering + one, entering)
        starts = [entering[:, t * wide : (t + 1) * wide] for t in range(strips)]

        def finish(k, starts):
            here = pl.ds(pl.multiple_of(k * rows, rows), rows)
            square = squares[k]
            leaving = []
            for strip in range(strips):
                b = lot * strips + strip
                grown = state_ref[b, here, :] + starts[strip]
                state = fall_buf[b, here, :] * grown
                state_ref[b, here, :] = state
                leaving.append(ends[b, k, :, :] * grown[rows - 1 : rows, :])
                for c in range(wide // 128):
                    part_state = state[:, c * 128 : (c + 1) * 128]
                    square = square + part_state * part_state
            squares[k] = square

            @pl.when(lot == lots - 1)
            def _():
                for step in range(1, m):
                    share(k, step).start()

            return tuple(leaving)

        lax.fori_loop(0, pieces, finish, tuple(starts))

    @pl.loop(0, pieces)
    def _(k):
        square = squares[k]
        for step in range(1, m):
            share(k, step).wait_recv()
            square = square + got_squares[step - 1, k]
        square_ref[pl.ds(pl.multiple_of(k * rows, rows), rows), :] = square
        for step in range(1, m):
            share(k, step).wait_send()

    @pl.loop(0, lots)
    def _(b):
        for step in range(1, group):
            tell_near(b, step).wait_send()

        @pl.loop(bunch + 1, bunches)
        def _(other):
            tell_far(b, other).wait_send()


def norm_kernel(length, channels, rows, state_ref, square_ref, norm_gain_ref, out_hbm, out_buf, sem):
    blocks, span, wide = state_ref.shape
    pieces = span // rows

    def put(k):
        here = pl.ds(pl.multiple_of(k * rows, rows), rows)
        return pltpu.make_async_copy(out_buf.at[k], out_hbm.at[0, here, :], sem.at[k])

    @pl.loop(0, pieces)
    def _(k):
        here = pl.ds(pl.multiple_of(k * rows, rows), rows)
        power = jnp.sum(square_ref[here, :], axis=1, keepdims=True) / (length * channels)
        gain = jnp.broadcast_to(lax.rsqrt(power + EPS) * length ** (-0.5), (rows, 128))
        for b in range(blocks):
            for c in range(wide // 128):
                columns = pl.ds(b * wide + c * 128, 128)
                state = state_ref[b, here, pl.ds(c * 128, 128)]
                out_buf[k, :, columns] = (state * gain * norm_gain_ref[:, columns]).astype(
                    out_buf.dtype
                )
        put(k).start()

    @pl.loop(0, pieces)
    def _(k):
        put(k).wait()


def per_device(n, m, fade_rate, update_in, norm_gain):
    _, span, own = fade_rate.shape
    length, channels = span * n, own * m
    wide, rows = piece_of(own, 256), piece_of(span, 128)
    group = group_of(n)
    broad, tall = piece_of(own, BROAD), piece_of(span, SLICE)
    lots, times = own // broad, span // tall
    blocks, pieces = own // wide, span // rows
    f32, bf16 = jnp.float32, jnp.bfloat16
    anywhere = pl.BlockSpec(memory_space=pl.ANY)
    in_vmem = pl.BlockSpec(memory_space=pltpu.VMEM)
    dma = pltpu.SemaphoreType.DMA
    state, square = pl.pallas_call(
        functools.partial(scan_kernel, n, m, length, wide, rows, group),
        out_shape=(
            pltpu.VMEM((blocks, span, wide), f32),
            pltpu.VMEM((span, 128), f32),
        ),
        in_specs=[anywhere, anywhere],
        out_specs=(in_vmem, in_vmem),
        scratch_shapes=[
            pltpu.VMEM((lots, span, broad), f32),
            pltpu.VMEM((lots, span, broad), bf16),
            pltpu.VMEM((blocks, span, wide), f32),
            pltpu.VMEM((rows, 2 * rows), bf16),
            pltpu.VMEM((blocks, pieces, 1, wide), f32),
            pltpu.VMEM((lots, 2, broad), f32),
            pltpu.VMEM((lots, group - 1, 2, broad), f32),
            pltpu.VMEM((lots, 2, broad), f32),
            pltpu.VMEM((lots, n // group, 2, broad), f32),
            pltpu.VMEM((pieces, rows, 128), f32),
            pltpu.VMEM((m - 1, pieces, rows, 128), f32),
            dma((lots * times,)),
            dma((lots * times,)),
            dma((lots, group - 1)),
            dma((lots, group - 1)),
            dma((lots, n // group)),
            dma((lots, n // group)),
            dma((m - 1, pieces)),
            dma((m - 1, pieces)),
        ],
        compiler_params=pltpu.CompilerParams(
            collective_id=0, has_side_effects=True, vmem_limit_bytes=44 * 2**20
        ),
        name="scan",
    )(fade_rate, update_in)
    return pl.pallas_call(
        functools.partial(norm_kernel, length, channels, rows),
        out_shape=jax.ShapeDtypeStruct((1, span, own), bf16),
        in_specs=[in_vmem, in_vmem, in_vmem],
        out_specs=anywhere,
        scratch_shapes=[pltpu.VMEM((pieces, rows, own), bf16), dma((pieces,))],
        compiler_params=pltpu.CompilerParams(vmem_limit_bytes=24 * 2**20),
        name="norm",
    )(state, square, norm_gain.reshape(1, own))


def solution(mesh):
    placed = (P(None, "sp", "tp"), P(None, "sp", "tp"), P("tp"))
    return jax.shard_map(
        functools.partial(per_device, mesh.shape["sp"], mesh.shape["tp"]),
        mesh=mesh, in_specs=placed, out_specs=P(None, "sp", "tp"), check_vma=False,
    )
```

```python
import functools

import jax
import jax.numpy as jnp
from jax import lax
from jax.experimental import pallas as pl
from jax.experimental.pallas import tpu as pltpu
from jax.sharding import PartitionSpec as P

MESH = pl.DeviceIdType.MESH
EPS = 1e-06
AHEAD = 8
BROAD = 1024
SLICE = 256


def piece_of(size, most):
    most = min(size, most)
    while size % most:
        most //= 2
    return most


def group_of(n):
    group = 1
    while group * group < n:
        group *= 2
    return group


def scan_kernel(
    n, m, length, wide, rows, group,
    fade_hbm, update_hbm, state_ref, square_ref,
    fade_buf, update_buf, fall_buf, tri, ends, summary, near, passed, far, squares, got_squares,
    fade_sem, update_sem, near_send, near_recv, far_send, far_recv, sq_send_sem, sq_recv_sem,
):
    me, part = lax.axis_index("sp"), lax.axis_index("tp")
    blocks, span, _ = state_ref.shape
    pieces = span // rows
    lots, _, broad = fade_buf.shape
    strips, times = broad // wide, fade_sem.shape[0] // lots
    tall = span // times
    bunches = n // group
    bunch, rank = me // group, lax.rem(me, group)

    def fetch(i):
        lot, time = i // times, lax.rem(i, times)
        here = pl.ds(pl.multiple_of(time * tall, tall), tall)
        columns = pl.ds(pl.multiple_of(lot * broad, broad), broad)
        return (
            pltpu.make_async_copy(
                fade_hbm.at[0, here, columns], fade_buf.at[lot, here, :], fade_sem.at[i]
            ),
            pltpu.make_async_copy(
                update_hbm.at[0, here, columns], update_buf.at[lot, here, :], update_sem.at[i]
            ),
        )

    ahead = min(AHEAD, lots * times)
    for i in range(ahead):
        for copy in fetch(jnp.int32(i)):
            copy.start()

    barrier = pltpu.get_barrier_semaphore()
    for step in range(1, group):
        other = bunch * group + lax.rem(rank + step, group)
        pl.semaphore_signal(barrier, inc=1, device_id=(other, part), device_id_type=MESH)
    for step in range(1, bunches):
        other = lax.rem(me + step * group, n)
        pl.semaphore_signal(barrier, inc=1, device_id=(other, part), device_id_type=MESH)
    for step in range(1, m):
        other = lax.rem(part + step, m)
        pl.semaphore_signal(barrier, inc=1, device_id=(me, other), device_id_type=MESH)

    later = lax.broadcasted_iota(jnp.int32, (rows, 2 * rows), 0)
    sooner = lax.rem(lax.broadcasted_iota(jnp.int32, (rows, 2 * rows), 1), rows)
    tri[...] = jnp.where(sooner <= later, 1.0, 0.0).astype(jnp.bfloat16)

    def tell_near(b, step):
        other = bunch * group + lax.rem(rank + step, group)
        return pltpu.make_async_remote_copy(
            src_ref=summary.at[b],
            dst_ref=near.at[b, step - 1],
            send_sem=near_send.at[b, step - 1],
            recv_sem=near_recv.at[b, step - 1],
            device_id=(other, part),
            device_id_type=MESH,
        )

    def tell_far(b, other):
        return pltpu.make_async_remote_copy(
            src_ref=passed.at[b],
            dst_ref=far.at[b, bunch],
            send_sem=far_send.at[b, other],
            recv_sem=far_recv.at[b, bunch],
            device_id=(other * group + rank, part),
            device_id_type=MESH,
        )

    def hear_far(b, other):
        return pltpu.make_async_remote_copy(
            src_ref=passed.at[b],
            dst_ref=far.at[b, other],
            send_sem=far_send.at[b, other],
            recv_sem=far_recv.at[b, other],
            device_id=(lax.rem(me + group, n), part),
            device_id_type=MESH,
        )

    def dot(a, b):
        return jnp.dot(a, b, preferred_element_type=jnp.float32)

    rate = 1.4426950408889634 / length

    summary[:, 0:1, :] = jnp.ones((lots, 1, broad), jnp.float32)
    summary[:, 1:2, :] = jnp.zeros((lots, 1, broad), jnp.float32)

    @pl.loop(0, lots * times)
    def _(i):
        for copy in fetch(i):
            copy.wait()

        @pl.when(i + ahead < lots * times)
        def _():
            for copy in fetch(i + ahead):
                copy.start()

        lot, time = i // times, lax.rem(i, times)
        for strip in range(strips):
            mine = slice(strip * wide, (strip + 1) * wide)
            b = lot * strips + strip
            total_fall, total = summary[lot, 0:1, mine], summary[lot, 1:2, mine]
            for k in range(tall // rows):
                here = pl.ds(pl.multiple_of(time * tall + k * rows, rows), rows)
                fade = fade_buf[lot, here, mine]
                faded = dot(tri[:, :rows], fade.astype(jnp.bfloat16)) * rate
                last_fall = jnp.exp2(jnp.sum(fade, axis=0, keepdims=True) * -rate)
                push = update_buf[lot, here, mine]
                extra = push.astype(jnp.float32) * (jnp.exp2(faded) - 1.0)
                both = jnp.concatenate([push, extra.astype(jnp.bfloat16)], axis=0)
                grown = dot(tri[...], both)
                fall_buf[b, here, :] = jnp.exp2(-faded)
                state_ref[b, here, :] = grown
                ends[b, time * (tall // rows) + k, :, :] = last_fall
                total = last_fall * (grown[rows - 1 : rows, :] + total)
                total_fall = total_fall * last_fall
            summary[lot, 0:1, mine] = total_fall
            summary[lot, 1:2, mine] = total

        @pl.when(i == times - 1)
        def _():
            pl.semaphore_wait(barrier, group + bunches + m - 3)

        @pl.when(time == times - 1)
        def _():
            for step in range(1, group):
                tell_near(lot, step).start()

    @pl.loop(0, lots)
    def _(b):
        for step in range(1, group):
            tell_near(b, step).wait_recv()

        fall = jnp.ones((1, broad), jnp.float32)
        value = jnp.zeros((1, broad), jnp.float32)
        for place in range(group):
            one_fall, one = summary[b, 0:1, :], summary[b, 1:2, :]
            for step in range(1, group):
                came = lax.rem(rank - place + group, group) == step
                one_fall = jnp.where(came, near[b, step - 1, 0:1, :], one_fall)
                one = jnp.where(came, near[b, step - 1, 1:2, :], one)
            fall = fall * one_fall
            value = one_fall * value + one
        passed[b, 0:1, :] = fall
        passed[b, 1:2, :] = value

        @pl.loop(bunch + 1, bunches)
        def _(other):
            tell_far(b, other).start()

    def share(k, step):
        other = lax.rem(part + step, m)
        return pltpu.make_async_remote_copy(
            src_ref=squares.at[k],
            dst_ref=got_squares.at[step - 1, k],
            send_sem=sq_send_sem.at[step - 1, k],
            recv_sem=sq_recv_sem.at[step - 1, k],
            device_id=(me, other),
            device_id_type=MESH,
        )

    squares[...] = jnp.zeros_like(squares)

    @pl.loop(0, lots)
    def _(lot):
        def take(other, entering):
            hear_far(lot, other).wait_recv()
            return far[lot, other, 0:1, :] * entering + far[lot, other, 1:2, :]

        entering = lax.fori_loop(0, bunch, take, jnp.zeros((1, broad), jnp.float32))
        for place in range(group - 1):
            one_fall, one = near[lot, 0, 0:1, :], near[lot, 0, 1:2, :]
            for step in range(2, group):
                came = rank - place == step
                one_fall = jnp.where(came, near[lot, step - 1, 0:1, :], one_fall)
                one = jnp.where(came, near[lot, step - 1, 1:2, :], one)
            before = place < rank
            entering = jnp.where(before, one_fall * entering + one, entering)
        starts = [entering[:, t * wide : (t + 1) * wide] for t in range(strips)]

        def finish(k, starts):
            here = pl.ds(pl.multiple_of(k * rows, rows), rows)
            square = squares[k]
            leaving = []
            for strip in range(strips):
                b = lot * strips + strip
                grown = state_ref[b, here, :] + starts[strip]
                state = fall_buf[b, here, :] * grown
                state_ref[b, here, :] = state
                leaving.append(ends[b, k, :, :] * grown[rows - 1 : rows, :])
                for c in range(wide // 128):
                    part_state = state[:, c * 128 : (c + 1) * 128]
                    square = square + part_state * part_state
            squares[k] = square

            @pl.when(lot == lots - 1)
            def _():
                for step in range(1, m):
                    share(k, step).start()

            return tuple(leaving)

        lax.fori_loop(0, pieces, finish, tuple(starts))

    @pl.loop(0, pieces)
    def _(k):
        square = squares[k]
        for step in range(1, m):
            share(k, step).wait_recv()
            square = square + got_squares[step - 1, k]
        square_ref[pl.ds(pl.multiple_of(k * rows, rows), rows), :] = square
        for step in range(1, m):
            share(k, step).wait_send()

    @pl.loop(0, lots)
    def _(b):
        for step in range(1, group):
            tell_near(b, step).wait_send()

        @pl.loop(bunch + 1, bunches)
        def _(other):
            tell_far(b, other).wait_send()


def norm_kernel(length, channels, rows, state_ref, square_ref, norm_gain_ref, out_hbm, out_buf, sem):
    blocks, span, wide = state_ref.shape
    pieces = span // rows

    def put(k):
        here = pl.ds(pl.multiple_of(k * rows, rows), rows)
        return pltpu.make_async_copy(out_buf.at[k], out_hbm.at[0, here, :], sem.at[k])

    @pl.loop(0, pieces)
    def _(k):
        here = pl.ds(pl.multiple_of(k * rows, rows), rows)
        power = jnp.sum(square_ref[here, :], axis=1, keepdims=True) / (length * channels)
        gain = jnp.broadcast_to(lax.rsqrt(power + EPS) * length ** (-0.5), (rows, 128))
        for b in range(blocks):
            for c in range(wide // 128):
                columns = pl.ds(b * wide + c * 128, 128)
                state = state_ref[b, here, pl.ds(c * 128, 128)]
                out_buf[k, :, columns] = (state * gain * norm_gain_ref[:, columns]).astype(
                    out_buf.dtype
                )
        put(k).start()

    @pl.loop(0, pieces)
    def _(k):
        put(k).wait()


def per_device(n, m, fade_rate, update_in, norm_gain):
    _, span, own = fade_rate.shape
    length, channels = span * n, own * m
    wide, rows = piece_of(own, 256), piece_of(span, 128)
    group = group_of(n)
    broad, tall = piece_of(own, BROAD), piece_of(span, SLICE)
    lots, times = own // broad, span // tall
    blocks, pieces = own // wide, span // rows
    f32, bf16 = jnp.float32, jnp.bfloat16
    anywhere = pl.BlockSpec(memory_space=pl.ANY)
    in_vmem = pl.BlockSpec(memory_space=pltpu.VMEM)
    dma = pltpu.SemaphoreType.DMA
    state, square = pl.pallas_call(
        functools.partial(scan_kernel, n, m, length, wide, rows, group),
        out_shape=(
            pltpu.VMEM((blocks, span, wide), f32),
            pltpu.VMEM((span, 128), f32),
        ),
        in_specs=[anywhere, anywhere],
        out_specs=(in_vmem, in_vmem),
        scratch_shapes=[
            pltpu.VMEM((lots, span, broad), f32),
            pltpu.VMEM((lots, span, broad), bf16),
            pltpu.VMEM((blocks, span, wide), f32),
            pltpu.VMEM((rows, 2 * rows), bf16),
            pltpu.VMEM((blocks, pieces, 1, wide), f32),
            pltpu.VMEM((lots, 2, broad), f32),
            pltpu.VMEM((lots, group - 1, 2, broad), f32),
            pltpu.VMEM((lots, 2, broad), f32),
            pltpu.VMEM((lots, n // group, 2, broad), f32),
            pltpu.VMEM((pieces, rows, 128), f32),
            pltpu.VMEM((m - 1, pieces, rows, 128), f32),
            dma((lots * times,)),
            dma((lots * times,)),
            dma((lots, group - 1)),
            dma((lots, group - 1)),
            dma((lots, n // group)),
            dma((lots, n // group)),
            dma((m - 1, pieces)),
            dma((m - 1, pieces)),
        ],
        compiler_params=pltpu.CompilerParams(
            collective_id=0, has_side_effects=True, vmem_limit_bytes=44 * 2**20
        ),
        name="scan",
    )(fade_rate, update_in)
    return pl.pallas_call(
        functools.partial(norm_kernel, length, channels, rows),
        out_shape=jax.ShapeDtypeStruct((1, span, own), bf16),
        in_specs=[in_vmem, in_vmem, in_vmem],
        out_specs=anywhere,
        scratch_shapes=[pltpu.VMEM((pieces, rows, own), bf16), dma((pieces,))],
        compiler_params=pltpu.CompilerParams(vmem_limit_bytes=24 * 2**20),
        name="norm",
    )(state, square, norm_gain.reshape(1, own))


def solution(mesh):
    placed = (P(None, "sp", "tp"), P(None, "sp", "tp"), P("tp"))
    return jax.shard_map(
        functools.partial(per_device, mesh.shape["sp"], mesh.shape["tp"]),
        mesh=mesh, in_specs=placed, out_specs=P(None, "sp", "tp"), check_vma=False,
    )
```
